256 devices in a mesh: tm: 16 (over x, y), row: 4 (over z_lo, core), col: 4 (over z_hi).
Axes of the slice: x: 4, y: 4, z: 8 (z_hi: 4, z_lo: 2; z = z_hi * 2 + z_lo), core: 2. Of those that a mesh axis runs over, the one named last changes fastest.
Arguments:
- returns: bfloat16 [11520, 4096], P('tm', ('row', 'col')), may hold values from -50 to 50
- block_bars: int32 [64], replicated, may hold values from 90 to 180
Outputs:
- correlation: bfloat16 [64, 4096, 4096], P('tm', 'row', 'col')
The draws below stay inside these ranges and needn't reach their ends.
All inputs are finite; a program needn't handle non-finite values.
Results may differ from the reference program's by a relative error of at most 0.0034.
Values may be sent and summed in bfloat16 or wider, within the bound.
No kernel may reach another device: no remote copies, remote signals or barrier semaphores. Data moves between devices by JAX's collectives and lax.ppermute only.
A program may use at most 128 MiB of HBM per device.

```python
import jax
import jax.numpy as jnp
from jax import lax

S = 4096
BLK = 180
NBLK = 64


def draw_returns(key, part):
    keys = jax.random.split(jax.random.fold_in(key, 7), 4)
    nrows = NBLK * BLK
    scales = jnp.exp(jax.random.uniform(keys[0], (1, S), jnp.float32, 0.0, jnp.log(10.0)))
    betas = jax.random.uniform(keys[1], (1, S), jnp.float32, -1.0, 1.0)
    factor = jax.random.normal(keys[2], (nrows, 1), jnp.float32)
    noise = jax.random.normal(keys[3], (nrows, S), jnp.float32)
    values = jnp.clip((betas * factor + noise) * scales, -50.0, 50.0)
    return values.astype(jnp.bfloat16)


def touch_ends(values, rng, low, largest):
    extent = values.shape
    index_at = [jax.random.randint(jax.random.fold_in(rng, axis), (), 0, extent[axis]) for axis in range(len(extent))]
    values = values.at[tuple(index_at)].set(low)
    longest = extent.index(max(extent))
    index_at[longest] = (index_at[longest] + 1) % extent[longest]
    return values.at[tuple(index_at)].set(largest)


def setup_inputs(seed: int = 0) -> dict:
    key_list = jax.random.split(jax.random.key(seed), 3)
    return {
        "returns": draw_returns(jax.random.fold_in(key_list[2], 71), 0),
        "block_bars": touch_ends(jax.random.randint(key_list[1], (NBLK,), BLK // 2, BLK + 1), jax.random.fold_in(key_list[1], 1), BLK // 2, BLK).astype(jnp.int32),
    }


def reference(returns, block_bars):
    blocks = returns.reshape(NBLK, BLK, S)

    def advance(carry, item):
        mean_prev, gram_prev, var_prev, count_prev = carry
        rows, count = item
        count_f = count.astype(jnp.float32)
        mask = (jnp.arange(BLK, dtype=jnp.int32)[:, None] < count).astype(jnp.float32)
        values = rows.astype(jnp.float32)
        mean_now = lax.optimization_barrier(jnp.sum(mask * values, axis=0)) / count_f
        centered = (mask * (values - mean_now[None, :])).astype(jnp.bfloat16)
        gram_now = jnp.dot(centered.T, centered, preferred_element_type=jnp.float32)
        cent_f = centered.astype(jnp.float32)
        var_now = lax.optimization_barrier(jnp.sum(cent_f * cent_f, axis=0))
        weight = count_prev * count_f / (count_prev + count_f)
        delta = mean_prev - mean_now
        cov = gram_prev + gram_now + weight * delta[:, None] * delta[None, :]
        var_all = var_prev + var_now + weight * delta * delta
        inverse = lax.rsqrt(var_all)
        corr = (cov * inverse[:, None] * inverse[None, :]).astype(jnp.bfloat16)
        return ((mean_now, gram_now, var_now, count_f), corr)
    start = (jnp.zeros((S,), jnp.float32), jnp.zeros((S, S), jnp.float32), jnp.zeros((S,), jnp.float32), jnp.zeros((), jnp.float32))
    final, output = lax.scan(advance, start, (blocks, block_bars))
    return output
```

```python
import functools

import jax
import jax.numpy as jnp
from jax import lax
from jax.experimental import pallas as pl
from jax.experimental.pallas import tpu as pltpu
from jax.sharding import PartitionSpec as P

BLK = 180
PAD = 192
W = 256
ZS = 8
GROUP = ("row", "col")


def lead(block):
    return (block * BLK) % 16


def stat_rows(first):
    spare = [*range(first), *range(first + BLK, PAD)]
    return spare[:6]


def member(z, core):
    return (2 * (z % 2) + core) * 4 + z // 2


def hop(x, step):
    route = [
        (member(z, k), member((z + step) % ZS, k)) for z in range(ZS) for k in range(2)
    ]
    return lax.ppermute(x, GROUP, route)


def to_partner(x):
    route = [
        (member(z, k), member(z, 1 - k)) for z in range(ZS) for k in range(2) if k == (z // 2) % 2
    ]
    return lax.ppermute(x, GROUP, route)


def three_parts(x):
    hi = x.astype(jnp.bfloat16).astype(jnp.float32)
    rest = x - hi
    mid = rest.astype(jnp.bfloat16).astype(jnp.float32)
    return hi, mid, rest - mid


def message(x, count, first):
    row = lax.broadcasted_iota(jnp.int32, (PAD, W), 0)
    bar = row - first
    keep = (bar >= 0) & (bar < count)
    x = jnp.where(keep, x.astype(jnp.float32), 0.0)
    divisor = jnp.full((1, W), jnp.maximum(count, 1).astype(jnp.float32))
    mean = jnp.sum(x, axis=0, keepdims=True) / divisor
    cent = jnp.where(keep, x - mean, 0.0).astype(jnp.bfloat16).astype(jnp.float32)
    square = jnp.sum(cent * cent, axis=0, keepdims=True)
    out = cent
    for at, part in zip(stat_rows(first), (*three_parts(mean), *three_parts(square))):
        out = jnp.where(row == at, part, out)
    return out.astype(jnp.bfloat16)


def prep_late(meta, bars, x_ref, out_ref):
    for i, b in enumerate((1, 2, 3)):
        first = lead(b)
        x = x_ref[b * BLK - first : b * BLK - first + PAD, :]
        out_ref[i * PAD : (i + 1) * PAD, :] = message(x, bars[meta[0] * 4 + b], first)


def prep_early(meta, bars, e_ref, x_ref, out_ref):
    tm = meta[0]
    before = jnp.where(tm > 0, bars[jnp.maximum(tm * 4 - 1, 0)], 0)
    out_ref[0:PAD, :] = message(e_ref[...], before, lead(3))
    out_ref[PAD : 2 * PAD, :] = message(x_ref[0:PAD, :], bars[tm * 4], 0)


def stats(ref, at, first):
    rows = stat_rows(first)
    parts = ref[at * PAD : (at + 1) * PAD, :].astype(jnp.float32)
    get = [parts[r : r + 1, :] for r in rows]
    return get[0] + get[1] + get[2], get[3] + get[4] + get[5]


def pair_stats(ref_a, at_a, first_a, ref_b, at_b, first_b, w):
    mean_a, sq_a = stats(ref_a, at_a, first_a)
    mean_b, sq_b = stats(ref_b, at_b, first_b)
    d = mean_a - mean_b
    total = sq_a + sq_b + w * d * d
    return d, lax.rsqrt(total)


def corr_kernel(plan, outs, n_in, meta, bars, *refs):
    sets = [refs[i * 4 : (i + 1) * 4] for i in range(n_in)]
    out_ref = refs[-6]
    lhs, col_of, row_of, stage, sems = refs[-5:]
    tm, c = meta[0], meta[1]
    n_sets = n_in // 2
    rows = sets[:n_sets]
    cols = sets[n_sets:]
    row_id = lax.broadcasted_iota(jnp.int32, (PAD, W), 0)
    for i, (s, at, blk) in enumerate(plan):
        first = lead(blk)
        keep = (row_id >= first) & (row_id < first + BLK)
        for m in range(4):
            x = rows[s][m][at * PAD : (at + 1) * PAD, :]
            x = jnp.where(keep, x.astype(jnp.float32), 0.0)
            lhs[m, i] = x.T.astype(jnp.bfloat16)
    for p in range(2):
        (sa, ata, ba), (sb, atb, bb) = plan[p], plan[p + 1]
        g = tm * 4 + outs[p]
        na = jnp.where(g > 0, bars[jnp.maximum(g - 1, 0)], 0).astype(jnp.float32)
        nb = bars[g].astype(jnp.float32)
        w = jnp.full((1, W), na * nb) / jnp.full((1, W), na + nb)
        for m in range(4):
            d, q = pair_stats(rows[sa][m], ata, lead(ba), rows[sb][m], atb, lead(bb), w)
            row_of[p, m] = jnp.concatenate(
                [w * d, q, jnp.zeros((6, W), jnp.float32)], axis=0
            ).T
            d, q = pair_stats(cols[sa][m], ata, lead(ba), cols[sb][m], atb, lead(bb), w)
            col_of[p, m] = jnp.concatenate([d, q, jnp.zeros((6, W), jnp.float32)], axis=0)

    def flush(slot):
        return pltpu.make_async_copy(
            stage.at[slot], out_ref.at[0, pl.ds(0, W), :], sems.at[slot]
        )

    for p in range(2):
        (sa, ata, _), (sb, atb, _) = plan[p], plan[p + 1]

        def row_chunk(mr, carry, p=p, sa=sa, ata=ata, sb=sb, atb=atb):
            slot = lax.rem(mr, 2)
            if p == 0:

                @pl.when(mr >= 2)
                def _():
                    flush(slot).wait()

            else:
                flush(slot).wait()
            wd = row_of[p, mr, :, 0:1]
            qi = row_of[p, mr, :, 1:2]
            left_a = lhs[mr, p]
            left_b = lhs[mr, p + 1]
            for mc in range(4):
                gram = jnp.dot(
                    left_a, cols[sa][mc][ata * PAD : (ata + 1) * PAD, :],
                    preferred_element_type=jnp.float32,
                ) + jnp.dot(
                    left_b, cols[sb][mc][atb * PAD : (atb + 1) * PAD, :],
                    preferred_element_type=jnp.float32,
                )
                d = col_of[p, mc, 0:1, :]
                qj = col_of[p, mc, 1:2, :]
                corr = (gram + wd * d) * qi * qj
                jc = lax.rem(c + 4 - mc, 4)
                stage[slot, :, pl.ds(pl.multiple_of(jc * W, W), W)] = corr.astype(jnp.bfloat16)
            jr = lax.rem(c + 4 - mr, 4)
            pltpu.make_async_copy(
                stage.at[slot],
                out_ref.at[outs[p], pl.ds(pl.multiple_of(jr * W, W), W), :],
                sems.at[slot],
            ).start()
            return carry

        lax.fori_loop(0, 4, row_chunk, 0)
    flush(0).wait()
    flush(1).wait()


SMEM = pl.BlockSpec(memory_space=pltpu.SMEM)
VMEM = pl.BlockSpec(memory_space=pltpu.VMEM)
ANY = pl.BlockSpec(memory_space=pl.ANY)


def correlate(plan, outs, meta, bars, sets, shape, into=None):
    operands = [x for group in sets for x in group]
    body = functools.partial(corr_kernel, plan, outs, len(sets))
    specs = [SMEM, SMEM] + [VMEM] * len(operands)
    aliases = {}
    if into is not None:
        inner = body

        def body(meta, bars, *refs):
            k = len(operands)
            inner(meta, bars, *refs[:k], *refs[k + 1 :])

        operands = operands + [into]
        specs = specs + [ANY]
        aliases = {len(specs) - 1: 0}
    return pl.pallas_call(
        body,
        out_shape=jax.ShapeDtypeStruct(shape, jnp.bfloat16),
        in_specs=specs,
        out_specs=ANY,
        input_output_aliases=aliases,
        scratch_shapes=[
            pltpu.VMEM((4, 3, W, PAD), jnp.bfloat16),
            pltpu.VMEM((2, 4, 8, W), jnp.float32),
            pltpu.VMEM((2, 4, W, 8), jnp.float32),
            pltpu.VMEM((2, W, 4 * W), jnp.bfloat16),
            pltpu.SemaphoreType.DMA((2,)),
        ],
    )(meta, bars, *operands)


def prep(body, meta, bars, arrays, blocks):
    return pl.pallas_call(
        body,
        out_shape=jax.ShapeDtypeStruct((blocks * PAD, W), jnp.bfloat16),
        in_specs=[SMEM, SMEM] + [VMEM] * len(arrays),
        out_specs=VMEM,
    )(meta, bars, *arrays)


def ring(x):
    got = {0: x}
    ahead, back = x, x
    for s in (1, 2, 3):
        ahead, back = hop(ahead, 1), hop(back, -1)
        got[s], got[ZS - s] = ahead, back
    half = x.shape[0] // 2
    got[4] = jnp.concatenate([hop(ahead[:half], 1), hop(back[half:], -1)], axis=0)
    return got


def tiles(got):
    row, col = lax.axis_index("row"), lax.axis_index("col")
    low, core = row // 2, row % 2
    shift = low - col // 2 + 1
    mine = core == col % 2
    cols = []
    for m in range(4):
        sel = lax.select_n(shift, got[(2 * m - 1) % ZS], got[2 * m], got[(2 * m + 1) % ZS])
        cols.append(jnp.where(mine, sel, to_partner(sel)))
    return [got[2 * m] for m in range(4)], cols


def on_device(returns, block_bars):
    nbars = returns.shape[0]
    nblocks = nbars // BLK
    tm = lax.axis_size("tm")
    meta = jnp.stack([lax.axis_index("tm"), lax.axis_index("col")]).astype(jnp.int32)
    earlier = lax.ppermute(returns[nbars - PAD :], "tm", [(i, i + 1) for i in range(tm - 1)])
    late = prep(prep_late, meta, block_bars, [returns], 3)
    early = prep(prep_early, meta, block_bars, [earlier, returns], 2)
    late_rows, late_cols = tiles(ring(late))
    early_rows, early_cols = tiles(ring(early))
    shape = (nblocks, 4 * W, 4 * W)
    out = correlate(
        [(0, 0, 1), (0, 1, 2), (0, 2, 3)], (2, 3), meta, block_bars, [late_rows, late_cols], shape
    )
    return correlate(
        [(0, 0, 3), (0, 1, 0), (1, 0, 1)],
        (0, 1),
        meta,
        block_bars,
        [early_rows, late_rows, early_cols, late_cols],
        shape,
        out,
    )


def solution(mesh):
    placed = (P("tm", ("row", "col")), P())
    return jax.shard_map(
        on_device, mesh=mesh, in_specs=placed, out_specs=P("tm", "row", "col"), check_vma=False
    )
```

```python
import functools

import jax
import jax.numpy as jnp
from jax import lax
from jax.experimental import pallas as pl
from jax.experimental.pallas import tpu as pltpu
from jax.sharding import PartitionSpec as P


BLK = 180
PAD = 192
W = 256
ZS = 8
GROUP = ("row", "col")


def lead(block):
    return (block * BLK) % 16


def stat_rows(first):
    spare = [*range(first), *range(first + BLK, PAD)]
    return spare[:6]


def member(z, core):
    return (2 * (z % 2) + core) * 4 + z // 2


def hop(x, step):
    route = [
        (member(z, k), member((z + step) % ZS, k)) for z in range(ZS) for k in range(2)
    ]
    return lax.ppermute(x, GROUP, route)


def to_partner(x):
    route = [
        (member(z, k), member(z, 1 - k)) for z in range(ZS) for k in range(2) if k == (z // 2) % 2
    ]
    return lax.ppermute(x, GROUP, route)


def three_parts(x):
    hi = x.astype(jnp.bfloat16).astype(jnp.float32)
    rest = x - hi
    mid = rest.astype(jnp.bfloat16).astype(jnp.float32)
    return hi, mid, rest - mid


def message(x, count, first):
    row = lax.broadcasted_iota(jnp.int32, (PAD, W), 0)
    bar = row - first
    keep = (bar >= 0) & (bar < count)
    x = jnp.where(keep, x.astype(jnp.float32), 0.0)
    divisor = jnp.full((1, W), jnp.maximum(count, 1).astype(jnp.float32))
    mean = jnp.sum(x, axis=0, keepdims=True) / divisor
    cent = jnp.where(keep, x - mean, 0.0).astype(jnp.bfloat16).astype(jnp.float32)
    square = jnp.sum(cent * cent, axis=0, keepdims=True)
    out = cent
    for at, part in zip(stat_rows(first), (*three_parts(mean), *three_parts(square))):
        out = jnp.where(row == at, part, out)
    return out.astype(jnp.bfloat16)


def prep_late(meta, bars, x_ref, out_ref):
    for i, b in enumerate((1, 2, 3)):
        first = lead(b)
        x = x_ref[b * BLK - first : b * BLK - first + PAD, :]
        out_ref[i * PAD : (i + 1) * PAD, :] = message(x, bars[meta[0] * 4 + b], first)


def prep_early(meta, bars, e_ref, x_ref, out_ref):
    tm = meta[0]
    before = jnp.where(tm > 0, bars[jnp.maximum(tm * 4 - 1, 0)], 0)
    out_ref[0:PAD, :] = message(e_ref[...], before, lead(3))
    out_ref[PAD : 2 * PAD, :] = message(x_ref[0:PAD, :], bars[tm * 4], 0)


def stats_of(block, first):
    part = block.astype(jnp.float32)
    get = [part[r : r + 1, :] for r in stat_rows(first)]
    return get[0] + get[1] + get[2], get[3] + get[4] + get[5]


def corr_kernel(plan, outs, n_pieces, meta, bars, *refs):
    ring_of = [refs[i * 12 : i * 12 + 8] for i in range(n_pieces)]
    sent_of = [refs[i * 12 + 8 : i * 12 + 12] for i in range(n_pieces)]
    out_ref = refs[-7]
    lhs, rhs, col_of, row_of, stage, sems = refs[-6:]
    tm, c, case = meta[0], meta[1], meta[2]
    row_id = lax.broadcasted_iota(jnp.int32, (PAD, W), 0)
    for k in range(4):

        @pl.when(case == k)
        def _(k=k):
            for i, (s, at, _) in enumerate(plan):
                for m in range(4):
                    src = sent_of[s][m] if k == 3 else ring_of[s][(2 * m + k - 1) % ZS]
                    rhs[i, m] = src[at * PAD : (at + 1) * PAD, :]

    for i, (s, at, blk) in enumerate(plan):
        first = lead(blk)
        keep = (row_id >= first) & (row_id < first + BLK)
        for m in range(4):
            x = ring_of[s][2 * m][at * PAD : (at + 1) * PAD, :]
            x = jnp.where(keep, x.astype(jnp.float32), 0.0)
            lhs[i, m * W : (m + 1) * W, :] = x.T.astype(jnp.bfloat16)

    for p in range(2):
        (sa, ata, ba), (sb, atb, bb) = plan[p], plan[p + 1]
        g = tm * 4 + outs[p]
        na = jnp.where(g > 0, bars[jnp.maximum(g - 1, 0)], 0).astype(jnp.float32)
        nb = bars[g].astype(jnp.float32)
        w = jnp.full((1, W), na * nb) / jnp.full((1, W), na + nb)

        def pair(xa, xb, ba=ba, bb=bb, w=w):
            mean_a, sq_a = stats_of(xa, lead(ba))
            mean_b, sq_b = stats_of(xb, lead(bb))
            d = mean_a - mean_b
            return d, lax.rsqrt(sq_a + sq_b + w * d * d)

        fill = jnp.zeros((6, W), jnp.float32)
        for m in range(4):
            xa = ring_of[sa][2 * m][ata * PAD : (ata + 1) * PAD, :]
            xb = ring_of[sb][2 * m][atb * PAD : (atb + 1) * PAD, :]
            d, q = pair(xa, xb)
            t = jnp.concatenate([w * d, q, fill], axis=0).T
            row_of[p, 0, m * W : (m + 1) * W, :] = jnp.broadcast_to(t[:, 0:1], (W, 128))
            row_of[p, 1, m * W : (m + 1) * W, :] = jnp.broadcast_to(t[:, 1:2], (W, 128))
            d, q = pair(rhs[p, m], rhs[p + 1, m])
            col_of[p, m] = jnp.concatenate([d, q, fill], axis=0)

    copies = []
    for p in range(2):
        for mr in range(4):
            r = slice(mr * W, (mr + 1) * W)
            for mc in range(4):
                gram = jnp.dot(
                    lhs[p, r, :], rhs[p, mc], preferred_element_type=jnp.float32
                ) + jnp.dot(lhs[p + 1, r, :], rhs[p + 1, mc], preferred_element_type=jnp.float32)
                jc = lax.rem(c + 4 - mc, 4)
                for h in (0, 128):
                    d = col_of[p, mc, 0:1, h : h + 128]
                    qj = col_of[p, mc, 1:2, h : h + 128]
                    corr = (gram[:, h : h + 128] + row_of[p, 0, r] * d) * row_of[p, 1, r] * qj
                    at = pl.multiple_of(jc * W + h, 128)
                    stage[p, r, pl.ds(at, 128)] = corr.astype(jnp.bfloat16)
            jr = lax.rem(c + 4 - mr, 4)
            copy = pltpu.make_async_copy(
                stage.at[p, r, :],
                out_ref.at[outs[p], pl.ds(pl.multiple_of(jr * W, W), W), :],
                sems.at[p * 4 + mr],
            )
            copy.start()
            copies.append(copy)
    for copy in copies:
        copy.wait()


SMEM = pl.BlockSpec(memory_space=pltpu.SMEM)
VMEM = pl.BlockSpec(memory_space=pltpu.VMEM)
ANY = pl.BlockSpec(memory_space=pl.ANY)


def correlate(plan, outs, meta, bars, pieces, shape, into=None):
    operands = [x for got, sent in pieces for x in (*[got[s] for s in range(ZS)], *sent)]
    body = functools.partial(corr_kernel, plan, outs, len(pieces))
    specs = [SMEM, SMEM] + [VMEM] * len(operands)
    aliases = {}
    if into is not None:
        inner, k = body, len(operands)

        def body(meta, bars, *refs):
            inner(meta, bars, *refs[:k], *refs[k + 1 :])

        operands = operands + [into]
        specs = specs + [ANY]
        aliases = {len(specs) - 1: 0}
    return pl.pallas_call(
        body,
        out_shape=jax.ShapeDtypeStruct(shape, jnp.bfloat16),
        in_specs=specs,
        out_specs=ANY,
        input_output_aliases=aliases,
        compiler_params=pltpu.CompilerParams(vmem_limit_bytes=18 * 2**20),
        scratch_shapes=[
            pltpu.VMEM((3, 4 * W, PAD), jnp.bfloat16),
            pltpu.VMEM((3, 4, PAD, W), jnp.bfloat16),
            pltpu.VMEM((2, 4, 8, W), jnp.float32),
            pltpu.VMEM((2, 2, 4 * W, 128), jnp.float32),
            pltpu.VMEM((2, 4 * W, 4 * W), jnp.bfloat16),
            pltpu.SemaphoreType.DMA((8,)),
        ],
    )(meta, bars, *operands)


def prep(body, meta, bars, arrays, blocks):
    return pl.pallas_call(
        body,
        out_shape=jax.ShapeDtypeStruct((blocks * PAD, W), jnp.bfloat16),
        in_specs=[SMEM, SMEM] + [VMEM] * len(arrays),
        out_specs=VMEM,
        compiler_params=pltpu.CompilerParams(vmem_limit_bytes=8 * 2**20),
    )(meta, bars, *arrays)


def gathered(x, last, shift):
    def swap(m):
        group = [got[(2 * m - 1) % ZS], got[2 * m], got[(2 * m + 1) % ZS]]
        group = lax.optimization_barrier(group)
        chosen = lax.select_n(shift, *group)
        return to_partner(chosen)

    got = {0: x}
    ahead, back = x, x
    for s in (1, 2, 3):
        ahead, back = hop(ahead, 1), hop(back, -1)
        ahead, back = lax.optimization_barrier((ahead, back))
        got[s], got[ZS - s] = ahead, back
    got[4] = hop(ahead if last > 0 else back, last)
    return got, [swap(m) for m in range(4)]


def on_device(returns, block_bars):
    nbars = returns.shape[0]
    nblocks = nbars // BLK
    tm = lax.axis_size("tm")
    row, col = lax.axis_index("row"), lax.axis_index("col")
    shift = row // 2 - col // 2 + 1
    case = jnp.where(row % 2 == col % 2, shift, 3)
    meta = jnp.stack([lax.axis_index("tm"), col, case]).astype(jnp.int32)
    earlier = lax.ppermute(returns[nbars - PAD :], "tm", [(i, i + 1) for i in range(tm - 1)])
    late = prep(prep_late, meta, block_bars, [returns], 3)
    early = prep(prep_early, meta, block_bars, [earlier, returns], 2)
    meta_b = jnp.maximum(meta, -1)
    late = gathered(late, 1, shift)
    early = gathered(early, -1, shift)
    shape = (nblocks, 4 * W, 4 * W)
    out = correlate([(0, 0, 1), (0, 1, 2), (0, 2, 3)], (2, 3), meta, block_bars, [late], shape)
    return correlate(
        [(0, 0, 3), (0, 1, 0), (1, 0, 1)], (0, 1), meta_b, block_bars, [early, late], shape, out
    )


def solution(mesh):
    placed = (P("tm", ("row", "col")), P())
    return jax.shard_map(
        on_device, mesh=mesh, in_specs=placed, out_specs=P("tm", "row", "col"), check_vma=False
    )
```

```python
import functools

import jax
import jax.numpy as jnp
from jax import lax
from jax.experimental import pallas as pl
from jax.experimental.pallas import tpu as pltpu
from jax.sharding import PartitionSpec as P


BLK = 180
PAD = 192
W = 256
ZS = 8
GROUP = ("row", "col")
LATE = (1, 2, 3)
NEAR = (0, 1, 3)


def lead(block):
    return (block * BLK) % 16


def stat_rows(first):
    spare = [*range(first), *range(first + BLK, PAD)]
    return spare[:6]


def member(z, core):
    return (2 * (z % 2) + core) * 4 + z // 2


def hop(x, step, needed=None):
    route = [
        (member(z, k), member((z + step) % ZS, k))
        for z in range(ZS)
        for k in range(2)
        if needed is None or ((z + step) % ZS, k) in needed
    ]
    return lax.ppermute(x, GROUP, route)


def to_partner(x):
    route = [
        (member(z, k), member(z, 1 - k)) for z in range(ZS) for k in range(2) if k == (z // 2) % 2
    ]
    return lax.ppermute(x, GROUP, route)


def three_parts(x):
    hi = x.astype(jnp.bfloat16).astype(jnp.float32)
    rest = x - hi
    mid = rest.astype(jnp.bfloat16).astype(jnp.float32)
    return hi, mid, rest - mid


def message(x, count, first):
    row = lax.broadcasted_iota(jnp.int32, (PAD, W), 0)
    bar = row - first
    keep = (bar >= 0) & (bar < count)
    x = jnp.where(keep, x.astype(jnp.float32), 0.0)
    divisor = jnp.full((1, W), jnp.maximum(count, 1).astype(jnp.float32))
    mean = jnp.sum(x, axis=0, keepdims=True) / divisor
    cent = jnp.where(keep, x - mean, 0.0).astype(jnp.bfloat16).astype(jnp.float32)
    square = jnp.sum(cent * cent, axis=0, keepdims=True)
    out = cent
    for at, part in zip(stat_rows(first), (*three_parts(mean), *three_parts(square))):
        out = jnp.where(row == at, part, out)
    return out.astype(jnp.bfloat16)


def block_count(meta, bars, b):
    at = meta[0] * 4 + b
    return jnp.where(at >= 0, bars[jnp.maximum(at, 0)], 0)


def prep_kernel(meta, bars_ref, x_ref, last_ref, late_ref, first_ref, x, bars, sems):
    copies = [
        pltpu.make_async_copy(bars_ref, bars, sems.at[0]),
        pltpu.make_async_copy(x_ref, x, sems.at[1]),
    ]
    for copy in copies:
        copy.start()
    for copy in copies:
        copy.wait()
    for b in (3, 1, 2, 0):
        first = lead(b)
        block = x[b * BLK - first : b * BLK - first + PAD, :]
        out = message(block, block_count(meta, bars, b), first)
        if b == 0:
            first_ref[...] = out
        else:
            late_ref[(b - 1) * PAD : b * PAD, :] = out
        if b == 3:
            last_ref[...] = out


def stats_of(block, first):
    part = block.astype(jnp.float32)
    get = [part[r : r + 1, :] for r in stat_rows(first)]
    return get[0] + get[1] + get[2], get[3] + get[4] + get[5]


def corr_kernel(blocks, pairs, far_at, n_in, meta, bars, *refs):
    n_pieces = n_in // 10
    ring_of = [refs[i * 10 : i * 10 + 8] for i in range(n_pieces)]
    sent_of = [refs[i * 10 + 8 : i * 10 + 10] for i in range(n_pieces)]
    out_ref = refs[-7]
    lhs, rhs, col_of, row_of, stage, sems = refs[-6:]
    c, case = meta[1], meta[2]
    row_id = lax.broadcasted_iota(jnp.int32, (PAD, W), 0)

    def row_block(i, m):
        piece, at, _ = blocks[i]
        return ring_of[piece][2 * m][at * PAD : (at + 1) * PAD, :]

    for k in range(4):

        @pl.when(case == k)
        def _(k=k):
            for i, (piece, at, _) in enumerate(blocks):
                for m in range(4):
                    src, lo = ring_of[piece][(2 * m + k - 1) % ZS], at * PAD
                    if k == 3 and m == 2:
                        src = sent_of[piece][1]
                        lo += far_at[piece]
                    elif k == 3:
                        src = sent_of[piece][0]
                        lo += NEAR.index(m) * (src.shape[0] // 3)
                    rhs[i, m] = src[lo : lo + PAD, :]

    for i, (_, _, blk) in enumerate(blocks):
        first = lead(blk % 4)
        keep = (row_id >= first) & (row_id < first + BLK)
        for m in range(4):
            x = jnp.where(keep, row_block(i, m).astype(jnp.float32), 0.0)
            lhs[i, m * W : (m + 1) * W, :] = x.T.astype(jnp.bfloat16)

    for p, (a, b, out) in enumerate(pairs):
        na = block_count(meta, bars, out - 1).astype(jnp.float32)
        nb = block_count(meta, bars, out).astype(jnp.float32)
        w = jnp.full((1, W), na * nb) / jnp.full((1, W), na + nb)

        def pair(xa, xb, a=a, b=b, w=w):
            mean_a, sq_a = stats_of(xa, lead(blocks[a][2] % 4))
            mean_b, sq_b = stats_of(xb, lead(blocks[b][2] % 4))
            d = mean_a - mean_b
            return d, lax.rsqrt(sq_a + sq_b + w * d * d)

        fill = jnp.zeros((6, W), jnp.float32)
        for m in range(4):
            d, q = pair(row_block(a, m), row_block(b, m))
            t = jnp.concatenate([w * d, q, fill], axis=0).T
            row_of[p, 0, m * W : (m + 1) * W, :] = jnp.broadcast_to(t[:, 0:1], (W, 128))
            row_of[p, 1, m * W : (m + 1) * W, :] = jnp.broadcast_to(t[:, 1:2], (W, 128))
            d, q = pair(rhs[a, m], rhs[b, m])
            col_of[p, m] = jnp.concatenate([d, q, fill], axis=0)

    copies = []
    for p, (a, b, out) in enumerate(pairs):
        for mr in range(4):
            r = slice(mr * W, (mr + 1) * W)
            for mc in range(4):
                gram = jnp.dot(
                    lhs[a, r, :], rhs[a, mc], preferred_element_type=jnp.float32
                ) + jnp.dot(lhs[b, r, :], rhs[b, mc], preferred_element_type=jnp.float32)
                jc = lax.rem(c + 4 - mc, 4)
                for h in (0, 128):
                    d = col_of[p, mc, 0:1, h : h + 128]
                    qj = col_of[p, mc, 1:2, h : h + 128]
                    corr = (gram[:, h : h + 128] + row_of[p, 0, r] * d) * row_of[p, 1, r] * qj
                    at = pl.multiple_of(jc * W + h, 128)
                    stage[p, r, pl.ds(at, 128)] = corr.astype(jnp.bfloat16)
            jr = lax.rem(c + 4 - mr, 4)
            copy = pltpu.make_async_copy(
                stage.at[p, r, :],
                out_ref.at[out, pl.ds(pl.multiple_of(jr * W, W), W), :],
                sems.at[p * 4 + mr],
            )
            copy.start()
            copies.append(copy)
    for copy in copies:
        copy.wait()


SMEM = pl.BlockSpec(memory_space=pltpu.SMEM)
HBM = pl.BlockSpec(memory_space=pltpu.HBM)
VMEM = pl.BlockSpec(memory_space=pltpu.VMEM)
ANY = pl.BlockSpec(memory_space=pl.ANY)


def correlate(blocks, pairs, far_at, meta, bars, pieces, shape):
    operands = [x for got, sent in pieces for x in (*[got[s] for s in range(ZS)], *sent)]
    nb, np = len(blocks), len(pairs)
    return pl.pallas_call(
        functools.partial(corr_kernel, blocks, pairs, far_at, len(operands)),
        out_shape=jax.ShapeDtypeStruct(shape, jnp.bfloat16),
        in_specs=[SMEM, SMEM] + [VMEM] * len(operands),
        out_specs=ANY,
        compiler_params=pltpu.CompilerParams(vmem_limit_bytes=26 * 2**20),
        scratch_shapes=[
            pltpu.VMEM((nb, 4 * W, PAD), jnp.bfloat16),
            pltpu.VMEM((nb, 4, PAD, W), jnp.bfloat16),
            pltpu.VMEM((np, 4, 8, W), jnp.float32),
            pltpu.VMEM((np, 2, 4 * W, 128), jnp.float32),
            pltpu.VMEM((np, 4 * W, 4 * W), jnp.bfloat16),
            pltpu.SemaphoreType.DMA((np * 4,)),
        ],
    )(meta, bars, *operands)


def prep(meta, bars, x):
    sizes = (PAD, len(LATE) * PAD, PAD)
    return pl.pallas_call(
        prep_kernel,
        out_shape=[jax.ShapeDtypeStruct((n, W), jnp.bfloat16) for n in sizes],
        in_specs=[SMEM, HBM, HBM],
        out_specs=[VMEM] * 3,
        compiler_params=pltpu.CompilerParams(vmem_limit_bytes=8 * 2**20),
        scratch_shapes=[
            pltpu.VMEM(x.shape, jnp.bfloat16),
            pltpu.SMEM(bars.shape, jnp.int32),
            pltpu.SemaphoreType.DMA((2,)),
        ],
    )(meta, *(pltpu.with_memory_space_constraint(v, pltpu.HBM) for v in (bars, x)))


CROSS = [
    (2 * c + low, c % 2) for c in range(4) for low in range(2) if low != c // 2
]


def gathered(x, last, shift, after=()):
    def pick(m, gate):
        group = [got[s % ZS] for s in (2 * m - 1, 2 * m, 2 * m + 1)]
        group = lax.optimization_barrier([*group, *gate])[:3]
        chosen = lax.select_n(shift, *group)
        return chosen

    got = {0: x}
    ahead, back = x, x
    for s in (1, 2, 3):
        ahead = hop(ahead, 1, CROSS if s == 3 and last < 0 else None)
        back = hop(back, -1, CROSS if s == 3 and last > 0 else None)
        if s < 3:
            ahead, back = lax.optimization_barrier((ahead, back))
        got[s], got[ZS - s] = ahead, back
    first = lax.optimization_barrier(pick(0, after[:1]))
    near = [first, *(pick(m, after[1:2]) for m in NEAR[1:])]
    near = jnp.concatenate(near, axis=0)
    got[4] = hop(ahead if last > 0 else back, last)
    far = pick(2, after[2:])
    return got, [near, far], [first, near, far]


def to_next(x):
    tm = lax.axis_size("tm")
    return lax.ppermute(x, "tm", [(i, i + 1) for i in range(tm - 1)])


def on_device(returns, block_bars):
    nblocks = returns.shape[0] // BLK
    row, col, tm_index = (lax.axis_index(name) for name in ("row", "col", "tm"))
    shift = row // 2 - col // 2 + 1
    mine = row % 2 == col % 2
    meta = jnp.stack([tm_index, col, jnp.where(mine, shift, 3)]).astype(jnp.int32)
    last, late, first = prep(meta, block_bars, returns)
    early = jnp.concatenate([to_next(last), first], axis=0)
    late, late_cols, gates = gathered(late, 1, shift)
    early, early_cols, _ = gathered(early, -1, shift, gates)
    far = jnp.concatenate([late_cols[1], early_cols[1]], axis=0)
    far = to_partner(far)
    late_sent = [to_partner(late_cols[0]), far]
    early_sent = [to_partner(early_cols[0]), far]
    return correlate(
        [(0, 2, 3), (0, 1, 2), (0, 0, 1), (1, 1, 0), (1, 0, -1)],
        [(1, 0, 3), (2, 1, 2), (3, 2, 1), (4, 3, 0)],
        [0, len(LATE) * PAD],
        meta,
        block_bars,
        [(late, late_sent), (early, early_sent)],
        (nblocks, 4 * W, 4 * W),
    )


def solution(mesh):
    placed = (P("tm", ("row", "col")), P())
    return jax.shard_map(
        on_device, mesh=mesh, in_specs=placed, out_specs=P("tm", "row", "col"), check_vma=False
    )
```
